32 devices in a mesh: grp: 2 (over y), row: 4 (over z), col: 4 (over x, core).
Axes of the slice: x: 2, y: 2, z: 4, core: 2. Of those that a mesh axis runs over, the one named last changes fastest.
Arguments:
- hessian_old: float32 [18432, 9216], P(('grp', 'row'), 'col'), parts along dimension 0, may hold values from -8 to 48, as said below
- tokens: bfloat16 [128, 9216], P(('grp', 'row'), 'col'), parts along dimension 0, may hold values from -6 to 6
- weight: float32 [128, 9216], P(('grp', 'row'), 'col'), parts along dimension 0, may hold values from -6 to 6
- dense_weight: float32 [128, 9216], P(('grp', 'row'), 'col'), parts along dimension 0, may hold values from -6 to 6
- block_mask: int32 [128, 72], P(('grp', 'row'), 'col'), parts along dimension 0, may hold values 0 or 1
Outputs:
- hessian: float32 [18432, 9216], P(('grp', 'row'), 'col'), parts along dimension 0
- new_weight: float32 [128, 9216], P(('grp', 'row'), 'col'), parts along dimension 0
The draws below stay inside these ranges and needn't reach their ends.
There are 2 independent parts, one for each index of `grp`. The reference program is written for one: setup_inputs(seed, part) draws one part's arguments, and reference() takes and returns one part's arrays. A program takes and returns all parts, laid end to end along the dimension named above; each array names one. Nothing has to cross between parts.
Inputs may be any that keep to these rules, and one draw needn't show every extreme that they name: hessian_old is symmetric and has a positive diagonal.
All inputs are finite; a program needn't handle non-finite values. No bound on the sum of `block_mask` on one device may be relied on, other than what follows from the above.
Results may differ from the reference program's by a relative error of at most 0.0035.
Values may be sent and summed in bfloat16 or wider, within the bound.
A program may use at most 128 MiB of HBM per device.

```python
import jax
import jax.numpy as jnp

W = 9216
BLOCK = 128
TOKENS = 64
R = 64
BLOCKS = 72


def draw_hessian_old(key, part):
    key_off = jax.random.fold_in(key, 11)
    key_diag = jax.random.fold_in(key, 12)
    loose = jax.random.normal(key_off, (W, W), jnp.float32) * 0.05
    symmetric = loose + loose.T
    diagonal_values = 0.5 * jnp.exp(jax.random.uniform(key_diag, (W,), jnp.float32, 0.0, jnp.log(8.0)))
    positions = jnp.arange(W)
    symmetric = symmetric.at[positions, positions].set(diagonal_values)
    return symmetric.astype(jnp.float32)


def plant(array, key, least, largest):
    longest = array.shape.index(max(array.shape))
    spots = []
    for shift in (0, 1):
        where = [jax.random.randint(jax.random.fold_in(key, axis), (), 0, length) for axis, length in enumerate(array.shape)]
        where[longest] = (where[longest] + shift) % array.shape[longest]
        spots.append(tuple(where))
    return array.at[spots[0]].set(least).at[spots[1]].set(largest)


def steps_of(stream_key, dims, cuts, least, high):
    def one(position, blocks):
        heights = jax.random.uniform(jax.random.fold_in(jax.random.fold_in(stream_key, 6), position), (blocks,), jnp.float32, least / len(cuts), high / len(cuts))
        return jnp.repeat(jnp.exp(heights), dims[position] // blocks).reshape((-1,) + (1,) * (len(dims) - position - 1))

    level = one(*cuts[0])
    for cut in cuts[1:]:
        level = level * one(*cut)
    return level


def scatter_about(own_key, dims, scale, bound, cuts=(), held_as=jnp.bfloat16):
    level = steps_of(own_key, dims, cuts, -0.22, 0.18) if cuts else 1.0
    entries = jax.random.normal(own_key, dims, jnp.float32) * scale * level
    return jnp.minimum(jnp.maximum(entries, -bound), bound).astype(held_as)


def setup_inputs(seed: int = 0, part: int = 0) -> dict:
    seeds = jax.random.split(jax.random.key(seed), 6)
    part_keys = jax.random.split(jax.random.fold_in(seeds[5], part), 6)
    hessian_old = draw_hessian_old(jax.random.fold_in(jax.random.fold_in(seeds[5], part), 71), part)
    tokens = scatter_about(part_keys[1], (TOKENS, W), 1.0, 6.0, ((0, 4), (1, 4)))
    weight = scatter_about(part_keys[2], (R, W), 1.0, 6.0, ((0, 4), (1, 4)), jnp.float32)
    dense_weight = scatter_about(part_keys[3], (R, W), 1.0, 6.0, ((0, 4), (1, 4)), jnp.float32)
    block_mask = plant((jax.random.randint(part_keys[4], (R, BLOCKS), 0, 2) < 1).astype(jnp.int32), jax.random.fold_in(part_keys[4], 1), 0, 1)
    return {"hessian_old": hessian_old, "tokens": tokens, "weight": weight, "dense_weight": dense_weight, "block_mask": block_mask}


def reference(hessian_old, tokens, weight, dense_weight, block_mask):
    gram_tile = jnp.dot(tokens.T, tokens, preferred_element_type=jnp.float32)
    hessian = hessian_old + gram_tile / TOKENS
    kept_mask = jnp.repeat(block_mask.astype(jnp.float32), BLOCK, axis=1)
    difference = (kept_mask * weight - dense_weight).astype(jnp.bfloat16)
    hess_low = hessian.astype(jnp.bfloat16)
    gradient = jnp.dot(difference, hess_low, preferred_element_type=jnp.float32)
    diag_sum = jnp.trace(hessian)
    step_size = 0.25 * W / diag_sum
    new_weight = kept_mask * (weight - step_size * gradient)
    return hessian, new_weight
```

```python
import functools

import jax
import jax.numpy as jnp
from jax import lax
from jax.experimental import pallas as pl
from jax.experimental.pallas import tpu as pltpu
from jax.sharding import PartitionSpec as P

MESH = pl.DeviceIdType.MESH


def general(hessian_old, tokens, weight, dense_weight, block_mask):
    row_tile = hessian_old.shape[0]
    col_tile = hessian_old.shape[1]
    row_idx = lax.axis_index("row")
    col_idx = lax.axis_index("col")
    col_panel = lax.all_gather(tokens, "row", axis=0, tiled=True)
    features = lax.all_gather(tokens, "col", axis=1, tiled=True)
    row_panel = lax.all_to_all(features, "row", split_axis=1, concat_axis=0, tiled=True)
    gram_tile = lax.dot_general(
        row_panel, col_panel, (((0,), (0,)), ((), ())), preferred_element_type=jnp.float32
    )
    token_count = tokens.shape[0] * lax.axis_size("row")
    hessian = hessian_old + gram_tile / token_count
    row_ids = lax.broadcasted_iota(jnp.int32, (row_tile, col_tile), 0) + row_idx * row_tile
    col_ids = lax.broadcasted_iota(jnp.int32, (row_tile, col_tile), 1) + col_idx * col_tile
    local_trace = jnp.sum(jnp.where(row_ids == col_ids, hessian, jnp.float32(0.0)))
    diag_sum = lax.psum(local_trace, ("row", "col"))
    weight_rows = weight.shape[0]
    block_count = block_mask.shape[1]
    block_width = col_tile // block_count
    kept_mask = (
        block_mask.astype(jnp.float32)[:, :, None] * jnp.ones((1, 1, block_width), jnp.float32)
    ).reshape(weight_rows, col_tile)
    difference = (kept_mask * weight - dense_weight).astype(jnp.bfloat16)
    hess_low = hessian.astype(jnp.bfloat16)
    partial_grad = lax.dot_general(
        lax.all_gather(difference, "row", axis=0, tiled=True),
        hess_low,
        (((1,), (1,)), ((), ())),
        preferred_element_type=jnp.float32,
    )
    spread = lax.all_to_all(partial_grad, "row", split_axis=0, concat_axis=1, tiled=True)
    gradient = lax.psum_scatter(spread, "col", scatter_dimension=1, tiled=True)
    step_size = 0.25 * (row_tile * lax.axis_size("row")) / diag_sum
    new_weight = kept_mask * (weight - step_size * gradient)
    return (hessian, new_weight)


def greet(devices):
    barrier = pltpu.get_barrier_semaphore()
    for device in devices:
        pl.semaphore_signal(barrier, inc=1, device_id=device, device_id_type=MESH)
    pl.semaphore_wait(barrier, len(devices))


def remote(src, dst, send_sem, recv_sem, device):
    return pltpu.make_async_remote_copy(
        src_ref=src, dst_ref=dst, send_sem=send_sem, recv_sem=recv_sem,
        device_id=device, device_id_type=MESH,
    )


def gather_kernel(
    n, tok_ref, w_ref, d_ref, m_ref, colp, rowt, rowd, diff,
    send_a, send_d, send_b, recv_a, recv_d, recv_b,
):
    g, r, c = lax.axis_index("grp"), lax.axis_index("row"), lax.axis_index("col")
    blocks = m_ref.shape[1]
    width = tok_ref.shape[1] // blocks
    for b in range(blocks):
        at = slice(b * width, (b + 1) * width)
        kept = m_ref[:, b : b + 1].astype(jnp.float32)
        diff[:, at] = (kept * w_ref[:, at] - d_ref[:, at]).astype(jnp.bfloat16)
    others = [lax.rem(r + j, n) for j in range(1, n)]
    beside = [lax.rem(c + j, n) for j in range(1, n)]
    greet([(g, rr, c) for rr in others] + [(g, r, cc) for cc in beside])

    root = r == c
    partner = c + 1 - 2 * lax.rem(c, 2)
    partner_dev = (g, r, partner)
    twins = [(g, r, lax.rem(c + 2 * j, n)) for j in range(1, n // 2)]
    even = lax.rem(r, 2) == lax.rem(c, 2)

    def token_copy(k):
        rr = lax.rem(c + k, n)
        return rr, remote(tok_ref, colp.at[r], send_a.at[k], recv_a.at[r], (g, rr, c))

    diff_copy = remote(diff, rowd.at[r], send_d, recv_d.at[r], (g, c, c))

    @pl.when(jnp.logical_not(root))
    def _():
        token_copy(0)[1].start()
        diff_copy.start()

    def spread(s, token_src, diff_src, devices, start):
        for i, device in enumerate(devices):
            one = remote(token_src, rowt.at[s], send_b.at[i, 0, s], recv_b.at[0, s], device)
            two = remote(diff_src, rowd.at[s], send_b.at[i, 1, s], recv_b.at[1, s], device)
            if start:
                one.start()
                two.start()
            else:
                one.wait_send()
                two.wait_send()

    @pl.when(root)
    def _():
        spread(r, tok_ref, diff, twins + [partner_dev], True)

    for k in range(1, n):
        rr, copy = token_copy(k)

        @pl.when(rr != r)
        def _():
            copy.start()

    colp[r] = tok_ref[...]

    def got_a(s):
        remote(tok_ref, colp.at[s], send_a.at[0], recv_a.at[s], partner_dev).wait_recv()

    def got_d(s):
        remote(diff, rowd.at[s], send_d, recv_d.at[s], partner_dev).wait_recv()

    def got_b(s):
        remote(tok_ref, rowt.at[s], send_d, recv_b.at[0, s], partner_dev).wait_recv()
        remote(diff, rowd.at[s], send_d, recv_b.at[1, s], partner_dev).wait_recv()

    @pl.when(root)
    def _():
        for s in others:
            got_a(s)
            got_d(s)
            spread(s, colp.at[s], rowd.at[s], twins + [partner_dev], True)
        rowd[r] = diff[...]
        for s in range(n):
            rowt[s] = colp[s]
        spread(r, tok_ref, diff, twins + [partner_dev], False)
        for s in others:
            spread(s, colp.at[s], rowd.at[s], twins + [partner_dev], False)

    @pl.when(jnp.logical_not(root))
    def _():
        @pl.when(even)
        def _():
            for s in [r] + others:
                got_b(s)
                spread(s, rowt.at[s], rowd.at[s], [partner_dev], True)
            for s in [r] + others:
                spread(s, rowt.at[s], rowd.at[s], [partner_dev], False)

        @pl.when(jnp.logical_not(even))
        def _():
            for s in [r] + others:
                got_b(s)

        for s in others:
            got_a(s)
        diff_copy.wait_send()

    for k in range(n):
        rr, copy = token_copy(k)

        @pl.when(rr != r)
        def _():
            copy.wait_send()


def main_kernel(n, token_count, old_ref, rt_ref, rd_ref, cp_ref, out_ref, part_ref, trace_ref, acc):
    i = pl.program_id(0)
    rows = old_ref.shape[0]

    @pl.when(i == 0)
    def _():
        acc[...] = jnp.zeros_like(acc)
        trace_ref[...] = jnp.zeros_like(trace_ref)

    gram = lax.dot_general(
        rt_ref[...], cp_ref[...], (((0,), (0,)), ((), ())), preferred_element_type=jnp.float32
    )
    hess = old_ref[...] + gram / token_count
    out_ref[...] = hess
    acc[...] += jnp.dot(rd_ref[...], hess.astype(jnp.bfloat16), preferred_element_type=jnp.float32)

    @pl.when(lax.axis_index("row") == lax.axis_index("col"))
    def _():
        square = out_ref[:, pl.ds(pl.multiple_of(i * rows, rows), rows)]
        same = lax.broadcasted_iota(jnp.int32, (rows, rows), 0) == lax.broadcasted_iota(
            jnp.int32, (rows, rows), 1
        )
        diag = jnp.where(same, square, 0.0)
        total = jnp.sum(diag.reshape(rows // 8, 8, rows), axis=0)
        for b in range(rows // 128):
            trace_ref[...] += total[:, b * 128 : (b + 1) * 128]

    @pl.when(i == pl.num_programs(0) - 1)
    def _():
        part_ref[...] = acc[...].astype(part_ref.dtype)


def step_kernel(n, size, part_ref, w_ref, m_ref, trace_ref, out_ref, got, traces, send_p, send_t, recv_p, recv_t):
    g, r, c = lax.axis_index("grp"), lax.axis_index("row"), lax.axis_index("col")
    others = [lax.rem(r + j, n) for j in range(1, n)]
    far = [
        (g, lax.rem(r + j, n), lax.rem(c + k, n)) for j in range(n) for k in range(n) if j or k
    ]
    greet(far)
    sends = [
        remote(part_ref.at[s], got.at[r], send_p.at[j], recv_p.at[r], (g, s, c))
        for j, s in enumerate(others)
    ]
    tells = [
        remote(trace_ref, traces.at[r], send_t.at[j], recv_t.at[r], device)
        for j, device in enumerate(far)
    ]

    @pl.when(r == c)
    def _():
        for copy in tells:
            copy.start()

    for copy in sends:
        copy.start()

    total = jnp.zeros(trace_ref.shape, jnp.float32)
    for s in range(n):
        @pl.when(jnp.logical_or(r != c, s != r))
        def _():
            remote(trace_ref, traces.at[s], send_t.at[0], recv_t.at[s], far[0]).wait_recv()

    @pl.when(r == c)
    def _():
        traces[r] = trace_ref[...]

    for s in range(n):
        total = total + traces[s]
    step = 0.25 * size / jnp.sum(total, axis=(0, 1), keepdims=True)
    for s in others:
        remote(part_ref.at[0], got.at[s], send_p.at[0], recv_p.at[s], far[0]).wait_recv()
    got[r] = part_ref[r]
    blocks = m_ref.shape[1]
    width = w_ref.shape[1] // blocks
    for b in range(blocks):
        at = slice(b * width, (b + 1) * width)
        grad = got[0, :, at].astype(jnp.float32)
        for s in range(1, n):
            grad = grad + got[s, :, at].astype(jnp.float32)
        kept = m_ref[:, b : b + 1].astype(jnp.float32)
        out_ref[:, at] = kept * (w_ref[:, at] - step * grad)
    for copy in sends:
        copy.wait_send()

    @pl.when(r == c)
    def _():
        for copy in tells:
            copy.wait_send()


def fused(n, hessian_old, tokens, weight, dense_weight, block_mask):
    tile = hessian_old.shape[0]
    held = tokens.shape[0]
    depth = weight.shape[0]
    vmem = pl.BlockSpec(memory_space=pltpu.VMEM)
    dma = pltpu.SemaphoreType.DMA
    colp, rowt, rowd = pl.pallas_call(
        functools.partial(gather_kernel, n),
        out_shape=(
            jax.ShapeDtypeStruct((n, held, tile), jnp.bfloat16),
            jax.ShapeDtypeStruct((n, held, tile), jnp.bfloat16),
            jax.ShapeDtypeStruct((n, depth, tile), jnp.bfloat16),
        ),
        in_specs=[vmem] * 4,
        out_specs=(vmem,) * 3,
        scratch_shapes=[
            pltpu.VMEM((depth, tile), jnp.bfloat16),
            dma((n,)),
            dma,
            dma((n // 2, 2, n)),
            dma((n,)),
            dma((n,)),
            dma((2, n)),
        ],
        compiler_params=pltpu.CompilerParams(
            collective_id=0, has_side_effects=True, vmem_limit_bytes=8 << 20
        ),
    )(tokens, weight, dense_weight, block_mask)
    colp = colp.reshape(n * held, tile)
    rowt = rowt.reshape(n * held, tile)
    rowd = rowd.reshape(n * depth, tile)
    rows = 256 if tile % 256 == 0 else 128
    hessian, partial, trace = pl.pallas_call(
        functools.partial(main_kernel, n, n * held),
        grid=(tile // rows,),
        out_shape=(
            jax.ShapeDtypeStruct((tile, tile), jnp.float32),
            jax.ShapeDtypeStruct((n * depth, tile), jnp.bfloat16),
            jax.ShapeDtypeStruct((8, 128), jnp.float32),
        ),
        in_specs=[
            pl.BlockSpec((rows, tile), lambda i: (i, 0)),
            pl.BlockSpec((n * held, rows), lambda i: (0, i)),
            pl.BlockSpec((n * depth, rows), lambda i: (0, i)),
            pl.BlockSpec((n * held, tile), lambda i: (0, 0)),
        ],
        out_specs=(
            pl.BlockSpec((rows, tile), lambda i: (i, 0)),
            pl.BlockSpec((n * depth, tile), lambda i: (0, 0)),
            pl.BlockSpec((8, 128), lambda i: (0, 0)),
        ),
        scratch_shapes=[pltpu.VMEM((n * depth, tile), jnp.float32)],
        compiler_params=pltpu.CompilerParams(vmem_limit_bytes=32 << 20),
    )(hessian_old, rowt, rowd, colp)
    new_weight = pl.pallas_call(
        functools.partial(step_kernel, n, tile * n),
        out_shape=jax.ShapeDtypeStruct((depth, tile), jnp.float32),
        in_specs=[vmem] * 4,
        out_specs=vmem,
        scratch_shapes=[
            pltpu.VMEM((n, depth, tile), jnp.bfloat16),
            pltpu.VMEM((n, 8, 128), jnp.float32),
            dma((n - 1,)),
            dma((n * n - 1,)),
            dma((n,)),
            dma((n,)),
        ],
        compiler_params=pltpu.CompilerParams(
            collective_id=1, has_side_effects=True, vmem_limit_bytes=8 << 20
        ),
    )(partial.reshape(n, depth, tile), weight, block_mask, trace)
    return hessian, new_weight


def solution(mesh):
    n = mesh.shape["row"]

    def on_device(hessian_old, tokens, weight, dense_weight, block_mask):
        tile = hessian_old.shape[0]
        fits = (
            n == mesh.shape["col"]
            and n > 1
            and n % 2 == 0
            and tile == hessian_old.shape[1]
            and tile % 128 == 0
            and tile == block_mask.shape[1] * 128
            and tokens.shape[0] % 16 == 0
            and weight.shape[0] % 16 == 0
        )
        args = (hessian_old, tokens, weight, dense_weight, block_mask)
        return fused(n, *args) if fits else general(*args)

    spec = P(("grp", "row"), "col")
    return jax.shard_map(
        on_device, mesh=mesh, in_specs=(spec,) * 5, out_specs=(spec, spec), check_vma=False
    )
```

```python
import functools

import jax
import jax.numpy as jnp
from jax import lax
from jax.experimental import pallas as pl
from jax.experimental.pallas import tpu as pltpu
from jax.sharding import PartitionSpec as P

MESH = pl.DeviceIdType.MESH


def general(hessian_old, tokens, weight, dense_weight, block_mask):
    row_tile = hessian_old.shape[0]
    col_tile = hessian_old.shape[1]
    row_idx = lax.axis_index("row")
    col_idx = lax.axis_index("col")
    col_panel = lax.all_gather(tokens, "row", axis=0, tiled=True)
    features = lax.all_gather(tokens, "col", axis=1, tiled=True)
    row_panel = lax.all_to_all(features, "row", split_axis=1, concat_axis=0, tiled=True)
    gram_tile = lax.dot_general(
        row_panel, col_panel, (((0,), (0,)), ((), ())), preferred_element_type=jnp.float32
    )
    token_count = tokens.shape[0] * lax.axis_size("row")
    hessian = hessian_old + gram_tile / token_count
    row_ids = lax.broadcasted_iota(jnp.int32, (row_tile, col_tile), 0) + row_idx * row_tile
    col_ids = lax.broadcasted_iota(jnp.int32, (row_tile, col_tile), 1) + col_idx * col_tile
    local_trace = jnp.sum(jnp.where(row_ids == col_ids, hessian, jnp.float32(0.0)))
    diag_sum = lax.psum(local_trace, ("row", "col"))
    weight_rows = weight.shape[0]
    block_count = block_mask.shape[1]
    block_width = col_tile // block_count
    kept_mask = (
        block_mask.astype(jnp.float32)[:, :, None] * jnp.ones((1, 1, block_width), jnp.float32)
    ).reshape(weight_rows, col_tile)
    difference = (kept_mask * weight - dense_weight).astype(jnp.bfloat16)
    hess_low = hessian.astype(jnp.bfloat16)
    partial_grad = lax.dot_general(
        lax.all_gather(difference, "row", axis=0, tiled=True),
        hess_low,
        (((1,), (1,)), ((), ())),
        preferred_element_type=jnp.float32,
    )
    spread = lax.all_to_all(partial_grad, "row", split_axis=0, concat_axis=1, tiled=True)
    gradient = lax.psum_scatter(spread, "col", scatter_dimension=1, tiled=True)
    step_size = 0.25 * (row_tile * lax.axis_size("row")) / diag_sum
    new_weight = kept_mask * (weight - step_size * gradient)
    return (hessian, new_weight)


def hail(devices):
    barrier = pltpu.get_barrier_semaphore()
    for device in devices:
        pl.semaphore_signal(barrier, inc=1, device_id=device, device_id_type=MESH)


def meet(count):
    pl.semaphore_wait(pltpu.get_barrier_semaphore(), count)


def remote(src, dst, send_sem, recv_sem, device):
    return pltpu.make_async_remote_copy(
        src_ref=src, dst_ref=dst, send_sem=send_sem, recv_sem=recv_sem,
        device_id=device, device_id_type=MESH,
    )


def gather_kernel(
    n, old_hbm, tok_hbm, w_hbm, d_hbm, m_hbm, old, colp, rowt, rowd, tok_ref, w_ref, d_ref, m_ref, diff,
    in_sem, send_a, send_d, send_b, recv_a, recv_d, recv_b,
):
    g, r, c = lax.axis_index("grp"), lax.axis_index("row"), lax.axis_index("col")
    loads = [
        pltpu.make_async_copy(src, dst, in_sem.at[i])
        for i, (src, dst) in enumerate(
            [(w_hbm, w_ref), (d_hbm, d_ref), (m_hbm, m_ref), (tok_hbm, tok_ref), (old_hbm, old)]
        )
    ]
    for load in loads:
        load.start()
    others = [lax.rem(r + j, n) for j in range(1, n)]
    beside = [lax.rem(c + j, n) for j in range(1, n)]
    hail([(g, rr, c) for rr in others] + [(g, r, cc) for cc in beside])
    for load in loads[:4]:
        load.wait()
    blocks = m_ref.shape[1]
    width = tok_ref.shape[1] // blocks
    for b in range(blocks):
        at = slice(b * width, (b + 1) * width)
        kept = m_ref[:, b : b + 1].astype(jnp.float32)
        diff[:, at] = (kept * w_ref[:, at] - d_ref[:, at]).astype(jnp.bfloat16)
    meet(len(others) + len(beside))

    root = r == c
    partner = c + 1 - 2 * lax.rem(c, 2)
    partner_dev = (g, r, partner)
    twins = [(g, r, lax.rem(c + 2 * j, n)) for j in range(1, n // 2)]
    even = lax.rem(r, 2) == lax.rem(c, 2)

    def token_copy(k):
        rr = lax.rem(c + k, n)
        return rr, remote(tok_ref, colp.at[r], send_a.at[k], recv_a.at[r], (g, rr, c))

    diff_copy = remote(diff, rowd.at[r], send_d, recv_d.at[r], (g, c, c))

    @pl.when(jnp.logical_not(root))
    def _():
        token_copy(0)[1].start()
        diff_copy.start()

    def spread(s, token_src, diff_src, devices, start):
        for i, device in enumerate(devices):
            one = remote(token_src, rowt.at[s], send_b.at[i, 0, s], recv_b.at[0, s], device)
            two = remote(diff_src, rowd.at[s], send_b.at[i, 1, s], recv_b.at[1, s], device)
            if start:
                one.start()
                two.start()
            else:
                one.wait_send()
                two.wait_send()

    @pl.when(root)
    def _():
        spread(r, tok_ref, diff, twins + [partner_dev], True)

    for k in range(1, n):
        rr, copy = token_copy(k)

        @pl.when(rr != r)
        def _():
            copy.start()

    colp[r] = tok_ref[...]

    def got_a(s):
        remote(tok_ref, colp.at[s], send_a.at[0], recv_a.at[s], partner_dev).wait_recv()

    def got_d(s):
        remote(diff, rowd.at[s], send_d, recv_d.at[s], partner_dev).wait_recv()

    def got_b(s):
        remote(tok_ref, rowt.at[s], send_d, recv_b.at[0, s], partner_dev).wait_recv()
        remote(diff, rowd.at[s], send_d, recv_b.at[1, s], partner_dev).wait_recv()

    @pl.when(root)
    def _():
        for s in others:
            got_a(s)
            got_d(s)
            spread(s, colp.at[s], rowd.at[s], twins + [partner_dev], True)
        rowd[r] = diff[...]
        for s in range(n):
            rowt[s] = colp[s]
        spread(r, tok_ref, diff, twins + [partner_dev], False)
        for s in others:
            spread(s, colp.at[s], rowd.at[s], twins + [partner_dev], False)

    @pl.when(jnp.logical_not(root))
    def _():
        @pl.when(even)
        def _():
            for s in [r] + others:
                got_b(s)
                spread(s, rowt.at[s], rowd.at[s], [partner_dev], True)
            for s in [r] + others:
                spread(s, rowt.at[s], rowd.at[s], [partner_dev], False)

        @pl.when(jnp.logical_not(even))
        def _():
            for s in [r] + others:
                got_b(s)

        for s in others:
            got_a(s)
        diff_copy.wait_send()

    for k in range(n):
        rr, copy = token_copy(k)

        @pl.when(rr != r)
        def _():
            copy.wait_send()

    loads[4].wait()


def main_kernel(
    n, rows, token_count, old_ref, rt_ref, rd_ref, cp_ref, out_hbm, part_ref, trace_ref, acc, out, out_sem
):
    tile = old_ref.shape[0]
    steps = tile // rows
    slots = out.shape[0]
    acc[...] = jnp.zeros_like(acc)
    trace_ref[...] = jnp.zeros_like(trace_ref)
    same = lax.broadcasted_iota(jnp.int32, (rows, rows), 0) == lax.broadcasted_iota(
        jnp.int32, (rows, rows), 1
    )

    def store(i):
        return pltpu.make_async_copy(
            out.at[lax.rem(i, slots)],
            out_hbm.at[pl.ds(pl.multiple_of(i * rows, rows), rows), :],
            out_sem.at[lax.rem(i, slots)],
        )

    @pl.loop(0, steps)
    def _(i):
        slot = lax.rem(i, slots)

        @pl.when(i >= slots)
        def _():
            store(i - slots).wait()

        here = pl.ds(pl.multiple_of(i * rows, rows), rows)
        gram = lax.dot_general(
            rt_ref[:, here], cp_ref[...], (((0,), (0,)), ((), ())), preferred_element_type=jnp.float32
        )
        hess = old_ref[here, :] + gram / token_count
        out[slot] = hess
        acc[...] += jnp.dot(
            rd_ref[:, here], hess.astype(jnp.bfloat16), preferred_element_type=jnp.float32
        )
        store(i).start()

        @pl.when(lax.axis_index("row") == lax.axis_index("col"))
        def _():
            diag = jnp.where(same, out[slot, :, here], 0.0)
            total = jnp.sum(diag.reshape(rows // 8, 8, rows), axis=0)
            for b in range(rows // 128):
                trace_ref[...] += total[:, b * 128 : (b + 1) * 128]

    part_ref[...] = acc[...].astype(part_ref.dtype)
    for k in range(min(slots, steps)):
        store(jnp.int32(steps - 1 - k)).wait()


def step_kernel(n, size, part_ref, w_ref, m_ref, trace_ref, out_ref, got, traces, send_p, send_t, recv_p, recv_t):
    g, r, c = lax.axis_index("grp"), lax.axis_index("row"), lax.axis_index("col")
    others = [lax.rem(r + j, n) for j in range(1, n)]
    far = [
        (g, lax.rem(r + j, n), lax.rem(c + k, n)) for j in range(n) for k in range(n) if j or k
    ]
    hail(far)
    meet(len(far))
    sends = [
        remote(part_ref.at[s], got.at[r], send_p.at[j], recv_p.at[r], (g, s, c))
        for j, s in enumerate(others)
    ]
    tells = [
        remote(trace_ref, traces.at[r], send_t.at[j], recv_t.at[r], device)
        for j, device in enumerate(far)
    ]

    @pl.when(r == c)
    def _():
        for copy in tells:
            copy.start()

    for copy in sends:
        copy.start()

    total = jnp.zeros(trace_ref.shape, jnp.float32)
    for s in range(n):
        @pl.when(jnp.logical_or(r != c, s != r))
        def _():
            remote(trace_ref, traces.at[s], send_t.at[0], recv_t.at[s], far[0]).wait_recv()

    @pl.when(r == c)
    def _():
        traces[r] = trace_ref[...]

    for s in range(n):
        total = total + traces[s]
    step = 0.25 * size / jnp.sum(total, axis=(0, 1), keepdims=True)
    for s in others:
        remote(part_ref.at[0], got.at[s], send_p.at[0], recv_p.at[s], far[0]).wait_recv()
    got[r] = part_ref[r]
    blocks = m_ref.shape[1]
    width = w_ref.shape[1] // blocks
    for b in range(blocks):
        at = slice(b * width, (b + 1) * width)
        grad = got[0, :, at].astype(jnp.float32)
        for s in range(1, n):
            grad = grad + got[s, :, at].astype(jnp.float32)
        kept = m_ref[:, b : b + 1].astype(jnp.float32)
        out_ref[:, at] = kept * (w_ref[:, at] - step * grad)
    for copy in sends:
        copy.wait_send()

    @pl.when(r == c)
    def _():
        for copy in tells:
            copy.wait_send()


def fused(n, hessian_old, tokens, weight, dense_weight, block_mask):
    tile = hessian_old.shape[0]
    held = tokens.shape[0]
    depth = weight.shape[0]
    vmem = pl.BlockSpec(memory_space=pltpu.VMEM)
    dma = pltpu.SemaphoreType.DMA
    hbm = pl.BlockSpec(memory_space=pltpu.HBM)
    old, colp, rowt, rowd = pl.pallas_call(
        functools.partial(gather_kernel, n),
        out_shape=(
            jax.ShapeDtypeStruct((tile, tile), jnp.float32),
            jax.ShapeDtypeStruct((n, held, tile), jnp.bfloat16),
            jax.ShapeDtypeStruct((n, held, tile), jnp.bfloat16),
            jax.ShapeDtypeStruct((n, depth, tile), jnp.bfloat16),
        ),
        in_specs=[hbm] * 5,
        out_specs=(vmem,) * 4,
        scratch_shapes=[
            pltpu.VMEM((held, tile), jnp.bfloat16),
            pltpu.VMEM((depth, tile), jnp.float32),
            pltpu.VMEM((depth, tile), jnp.float32),
            pltpu.VMEM(block_mask.shape, jnp.int32),
            pltpu.VMEM((depth, tile), jnp.bfloat16),
            dma((5,)),
            dma((n,)),
            dma,
            dma((n // 2, 2, n)),
            dma((n,)),
            dma((n,)),
            dma((2, n)),
        ],
        compiler_params=pltpu.CompilerParams(
            collective_id=0, has_side_effects=True, vmem_limit_bytes=4 << 20
        ),
    )(*[pltpu.with_memory_space_constraint(x, pltpu.HBM) for x in (hessian_old, tokens, weight, dense_weight, block_mask)])
    colp = colp.reshape(n * held, tile)
    rowt = rowt.reshape(n * held, tile)
    rowd = rowd.reshape(n * depth, tile)
    rows = 128
    hessian, partial, trace = pl.pallas_call(
        functools.partial(main_kernel, n, rows, n * held),
        out_shape=(
            jax.ShapeDtypeStruct((tile, tile), jnp.float32),
            jax.ShapeDtypeStruct((n * depth, tile), jnp.bfloat16),
            jax.ShapeDtypeStruct((8, 128), jnp.float32),
        ),
        in_specs=[vmem] * 4,
        out_specs=(hbm, vmem, vmem),
        scratch_shapes=[
            pltpu.VMEM((n * depth, tile), jnp.float32),
            pltpu.VMEM((4, rows, tile), jnp.float32),
            dma((4,)),
        ],
        compiler_params=pltpu.CompilerParams(vmem_limit_bytes=12 << 20),
    )(old, rowt, rowd, colp)
    new_weight = pl.pallas_call(
        functools.partial(step_kernel, n, tile * n),
        out_shape=jax.ShapeDtypeStruct((depth, tile), jnp.float32),
        in_specs=[vmem] * 4,
        out_specs=vmem,
        scratch_shapes=[
            pltpu.VMEM((n, depth, tile), jnp.bfloat16),
            pltpu.VMEM((n, 8, 128), jnp.float32),
            dma((n - 1,)),
            dma((n * n - 1,)),
            dma((n,)),
            dma((n,)),
        ],
        compiler_params=pltpu.CompilerParams(
            collective_id=1, has_side_effects=True, vmem_limit_bytes=8 << 20
        ),
    )(partial.reshape(n, depth, tile), weight, block_mask, trace)
    return hessian, new_weight


def solution(mesh):
    n = mesh.shape["row"]

    def on_device(hessian_old, tokens, weight, dense_weight, block_mask):
        tile = hessian_old.shape[0]
        fits = (
            n == mesh.shape["col"]
            and n > 1
            and n % 2 == 0
            and tile == hessian_old.shape[1]
            and tile % 128 == 0
            and tile == block_mask.shape[1] * 128
            and tokens.shape[0] % 16 == 0
            and weight.shape[0] % 16 == 0
        )
        args = (hessian_old, tokens, weight, dense_weight, block_mask)
        return fused(n, *args) if fits else general(*args)

    spec = P(("grp", "row"), "col")
    return jax.shard_map(
        on_device, mesh=mesh, in_specs=(spec,) * 5, out_specs=(spec, spec), check_vma=False
    )
```

```python
import functools

import jax
import jax.numpy as jnp
from jax import lax
from jax.experimental import pallas as pl
from jax.experimental.pallas import tpu as pltpu
from jax.sharding import PartitionSpec as P

MESH = pl.DeviceIdType.MESH


def general(hessian_old, tokens, weight, dense_weight, block_mask):
    row_tile = hessian_old.shape[0]
    col_tile = hessian_old.shape[1]
    row_idx = lax.axis_index("row")
    col_idx = lax.axis_index("col")
    col_panel = lax.all_gather(tokens, "row", axis=0, tiled=True)
    features = lax.all_gather(tokens, "col", axis=1, tiled=True)
    row_panel = lax.all_to_all(features, "row", split_axis=1, concat_axis=0, tiled=True)
    gram_tile = lax.dot_general(
        row_panel, col_panel, (((0,), (0,)), ((), ())), preferred_element_type=jnp.float32
    )
    token_count = tokens.shape[0] * lax.axis_size("row")
    hessian = hessian_old + gram_tile / token_count
    row_ids = lax.broadcasted_iota(jnp.int32, (row_tile, col_tile), 0) + row_idx * row_tile
    col_ids = lax.broadcasted_iota(jnp.int32, (row_tile, col_tile), 1) + col_idx * col_tile
    local_trace = jnp.sum(jnp.where(row_ids == col_ids, hessian, jnp.float32(0.0)))
    diag_sum = lax.psum(local_trace, ("row", "col"))
    weight_rows = weight.shape[0]
    block_count = block_mask.shape[1]
    block_width = col_tile // block_count
    kept_mask = (
        block_mask.astype(jnp.float32)[:, :, None] * jnp.ones((1, 1, block_width), jnp.float32)
    ).reshape(weight_rows, col_tile)
    difference = (kept_mask * weight - dense_weight).astype(jnp.bfloat16)
    hess_low = hessian.astype(jnp.bfloat16)
    partial_grad = lax.dot_general(
        lax.all_gather(difference, "row", axis=0, tiled=True),
        hess_low,
        (((1,), (1,)), ((), ())),
        preferred_element_type=jnp.float32,
    )
    spread = lax.all_to_all(partial_grad, "row", split_axis=0, concat_axis=1, tiled=True)
    gradient = lax.psum_scatter(spread, "col", scatter_dimension=1, tiled=True)
    step_size = 0.25 * (row_tile * lax.axis_size("row")) / diag_sum
    new_weight = kept_mask * (weight - step_size * gradient)
    return (hessian, new_weight)


def hail(devices):
    barrier = pltpu.get_barrier_semaphore()
    for device in devices:
        pl.semaphore_signal(barrier, inc=1, device_id=device, device_id_type=MESH)


def meet(count):
    pl.semaphore_wait(pltpu.get_barrier_semaphore(), count)


def remote(src, dst, send_sem, recv_sem, device):
    return pltpu.make_async_remote_copy(
        src_ref=src, dst_ref=dst, send_sem=send_sem, recv_sem=recv_sem,
        device_id=device, device_id_type=MESH,
    )


def gather_kernel(
    n, old_hbm, tok_hbm, w_hbm, d_hbm, m_hbm, old, colp, rowt, rowd, tok_ref, w_ref, d_ref, m_ref, diff,
    in_sem, send_a, send_d, send_b, send_r, recv_a, recv_d, recv_b,
):
    g, r, c = lax.axis_index("grp"), lax.axis_index("row"), lax.axis_index("col")
    loads = [
        pltpu.make_async_copy(src, dst, in_sem.at[i])
        for i, (src, dst) in enumerate(
            [(w_hbm, w_ref), (d_hbm, d_ref), (m_hbm, m_ref), (tok_hbm, tok_ref), (old_hbm, old)]
        )
    ]
    for load in loads:
        load.start()
    others = [lax.rem(r + j, n) for j in range(1, n)]
    beside = [lax.rem(c + j, n) for j in range(1, n)]
    hail([(g, rr, c) for rr in others] + [(g, r, cc) for cc in beside])
    for load in loads[:4]:
        load.wait()
    blocks = m_ref.shape[1]
    width = tok_ref.shape[1] // blocks
    for b in range(blocks):
        at = slice(b * width, (b + 1) * width)
        kept = m_ref[:, b : b + 1].astype(jnp.float32)
        diff[:, at] = (kept * w_ref[:, at] - d_ref[:, at]).astype(jnp.bfloat16)
    meet(len(others) + len(beside))

    root = r == c
    partner = c + 1 - 2 * lax.rem(c, 2)
    partner_dev = (g, r, partner)
    twins = [(g, r, lax.rem(c + 2 * j, n)) for j in range(1, n // 2)]
    even = lax.rem(r, 2) == lax.rem(c, 2)

    mate = partner
    crosses = r // 2 != c // 2

    def direct(rr):
        return jnp.logical_and(rr != r, jnp.logical_not(jnp.logical_and(crosses, rr == mate)))

    def relay(s):
        return s // 2 != r // 2, remote(
            colp.at[s], colp.at[s], send_r.at[s], recv_a.at[s], (g, mate, c)
        )

    def token_copy(k):
        rr = lax.rem(c + k, n)
        return rr, remote(tok_ref, colp.at[r], send_a.at[k], recv_a.at[r], (g, rr, c))

    diff_copy = remote(diff, rowd.at[r], send_d, recv_d.at[r], (g, c, c))

    @pl.when(jnp.logical_not(root))
    def _():
        token_copy(0)[1].start()
        diff_copy.start()

    def spread(s, token_src, diff_src, devices, start):
        for i, device in enumerate(devices):
            one = remote(token_src, rowt.at[s], send_b.at[i, 0, s], recv_b.at[0, s], device)
            two = remote(diff_src, rowd.at[s], send_b.at[i, 1, s], recv_b.at[1, s], device)
            if start:
                one.start()
                two.start()
            else:
                one.wait_send()
                two.wait_send()

    @pl.when(root)
    def _():
        spread(r, tok_ref, diff, twins + [partner_dev], True)

    for k in range(1, n):
        rr, copy = token_copy(k)

        @pl.when(direct(rr))
        def _():
            copy.start()

    colp[r] = tok_ref[...]

    def got_a(s):
        remote(tok_ref, colp.at[s], send_a.at[0], recv_a.at[s], partner_dev).wait_recv()

    def got_d(s):
        remote(diff, rowd.at[s], send_d, recv_d.at[s], partner_dev).wait_recv()

    def got_b(s):
        remote(tok_ref, rowt.at[s], send_d, recv_b.at[0, s], partner_dev).wait_recv()
        remote(diff, rowd.at[s], send_d, recv_b.at[1, s], partner_dev).wait_recv()

    @pl.when(root)
    def _():
        for s in others:
            got_a(s)
            got_d(s)
            spread(s, colp.at[s], rowd.at[s], twins + [partner_dev], True)
            far, copy = relay(s)

            @pl.when(far)
            def _():
                copy.start()

        rowd[r] = diff[...]
        for s in range(n):
            rowt[s] = colp[s]
        spread(r, tok_ref, diff, twins + [partner_dev], False)
        for s in others:
            spread(s, colp.at[s], rowd.at[s], twins + [partner_dev], False)
            far, copy = relay(s)

            @pl.when(far)
            def _():
                copy.wait_send()


    @pl.when(jnp.logical_not(root))
    def _():
        @pl.when(even)
        def _():
            for s in [r] + others:
                got_b(s)
                spread(s, rowt.at[s], rowd.at[s], [partner_dev], True)
            for s in [r] + others:
                spread(s, rowt.at[s], rowd.at[s], [partner_dev], False)

        @pl.when(jnp.logical_not(even))
        def _():
            for s in [r] + others:
                got_b(s)

        for s in others:
            got_a(s)
        diff_copy.wait_send()

    for k in range(n):
        rr, copy = token_copy(k)

        @pl.when(direct(rr))
        def _():
            copy.wait_send()

    loads[4].wait()


def scaled(value, count):
    exact = count & (count - 1) == 0
    return value * (1.0 / count) if exact else value / count


def main_kernel(
    n, rows, token_count, old_ref, rt_ref, rd_ref, cp_ref, out_hbm, part_ref, trace_ref, acc, out, out_sem
):
    tile = old_ref.shape[0]
    steps = tile // rows
    slots = out.shape[0]
    acc[...] = jnp.zeros_like(acc)
    trace_ref[...] = jnp.zeros_like(trace_ref)
    same = lax.broadcasted_iota(jnp.int32, (rows, rows), 0) == lax.broadcasted_iota(
        jnp.int32, (rows, rows), 1
    )

    def store(i):
        return pltpu.make_async_copy(
            out.at[lax.rem(i, slots)],
            out_hbm.at[pl.ds(pl.multiple_of(i * rows, rows), rows), :],
            out_sem.at[lax.rem(i, slots)],
        )

    @pl.loop(0, steps)
    def _(i):
        slot = lax.rem(i, slots)

        @pl.when(i >= slots)
        def _():
            store(i - slots).wait()

        here = pl.ds(pl.multiple_of(i * rows, rows), rows)
        gram = lax.dot_general(
            rt_ref[:, here], cp_ref[...], (((0,), (0,)), ((), ())), preferred_element_type=jnp.float32
        )
        hess = old_ref[here, :] + scaled(gram, token_count)
        out[slot] = hess
        acc[...] += jnp.dot(
            rd_ref[:, here], hess.astype(jnp.bfloat16), preferred_element_type=jnp.float32
        )
        store(i).start()

        @pl.when(lax.axis_index("row") == lax.axis_index("col"))
        def _():
            diag = jnp.where(same, out[slot, :, here], 0.0)
            total = jnp.sum(diag.reshape(rows // 8, 8, rows), axis=0)
            for b in range(rows // 128):
                trace_ref[...] += total[:, b * 128 : (b + 1) * 128]

    part_ref[...] = acc[...].astype(part_ref.dtype)
    for k in range(min(slots, steps)):
        store(jnp.int32(steps - 1 - k)).wait()


def step_kernel(n, size, part_ref, w_ref, m_ref, trace_ref, out_ref, got, traces, send_p, send_t, recv_p, recv_t):
    g, r, c = lax.axis_index("grp"), lax.axis_index("row"), lax.axis_index("col")
    others = [lax.rem(r + j, n) for j in range(1, n)]
    far = [
        (g, lax.rem(r + j, n), lax.rem(c + k, n)) for j in range(n) for k in range(n) if j or k
    ]
    hail(far)
    meet(len(far))
    sends = [
        remote(part_ref.at[s], got.at[r], send_p.at[j], recv_p.at[r], (g, s, c))
        for j, s in enumerate(others)
    ]
    tells = [
        remote(trace_ref, traces.at[r], send_t.at[j], recv_t.at[r], device)
        for j, device in enumerate(far)
    ]

    @pl.when(r == c)
    def _():
        for copy in tells:
            copy.start()

    for copy in sends:
        copy.start()

    total = jnp.zeros(trace_ref.shape, jnp.float32)
    for s in range(n):
        @pl.when(jnp.logical_or(r != c, s != r))
        def _():
            remote(trace_ref, traces.at[s], send_t.at[0], recv_t.at[s], far[0]).wait_recv()

    @pl.when(r == c)
    def _():
        traces[r] = trace_ref[...]

    for s in range(n):
        total = total + traces[s]
    step = 0.25 * size / jnp.sum(total, axis=(0, 1), keepdims=True)
    for s in others:
        remote(part_ref.at[0], got.at[s], send_p.at[0], recv_p.at[s], far[0]).wait_recv()
    got[r] = part_ref[r]
    blocks = m_ref.shape[1]
    width = w_ref.shape[1] // blocks
    for b in range(blocks):
        at = slice(b * width, (b + 1) * width)
        grad = got[0, :, at].astype(jnp.float32)
        for s in range(1, n):
            grad = grad + got[s, :, at].astype(jnp.float32)
        kept = m_ref[:, b : b + 1].astype(jnp.float32)
        out_ref[:, at] = kept * (w_ref[:, at] - step * grad)
    for copy in sends:
        copy.wait_send()

    @pl.when(r == c)
    def _():
        for copy in tells:
            copy.wait_send()


def fused(n, hessian_old, tokens, weight, dense_weight, block_mask):
    tile = hessian_old.shape[0]
    held = tokens.shape[0]
    depth = weight.shape[0]
    vmem = pl.BlockSpec(memory_space=pltpu.VMEM)
    dma = pltpu.SemaphoreType.DMA
    hbm = pl.BlockSpec(memory_space=pltpu.HBM)
    old, colp, rowt, rowd = pl.pallas_call(
        functools.partial(gather_kernel, n),
        out_shape=(
            jax.ShapeDtypeStruct((tile, tile), jnp.float32),
            jax.ShapeDtypeStruct((n, held, tile), jnp.bfloat16),
            jax.ShapeDtypeStruct((n, held, tile), jnp.bfloat16),
            jax.ShapeDtypeStruct((n, depth, tile), jnp.bfloat16),
        ),
        in_specs=[hbm] * 5,
        out_specs=(vmem,) * 4,
        scratch_shapes=[
            pltpu.VMEM((held, tile), jnp.bfloat16),
            pltpu.VMEM((depth, tile), jnp.float32),
            pltpu.VMEM((depth, tile), jnp.float32),
            pltpu.VMEM(block_mask.shape, jnp.int32),
            pltpu.VMEM((depth, tile), jnp.bfloat16),
            dma((5,)),
            dma((n,)),
            dma,
            dma((n // 2, 2, n)),
            dma((n,)),
            dma((n,)),
            dma((n,)),
            dma((2, n)),
        ],
        compiler_params=pltpu.CompilerParams(
            collective_id=0, has_side_effects=True, vmem_limit_bytes=4 << 20
        ),
    )(*[pltpu.with_memory_space_constraint(x, pltpu.HBM) for x in (hessian_old, tokens, weight, dense_weight, block_mask)])
    colp = colp.reshape(n * held, tile)
    rowt = rowt.reshape(n * held, tile)
    rowd = rowd.reshape(n * depth, tile)
    rows = 256 if tile % 256 == 0 else 128
    hessian, partial, trace = pl.pallas_call(
        functools.partial(main_kernel, n, rows, n * held),
        out_shape=(
            jax.ShapeDtypeStruct((tile, tile), jnp.float32),
            jax.ShapeDtypeStruct((n * depth, tile), jnp.bfloat16),
            jax.ShapeDtypeStruct((8, 128), jnp.float32),
        ),
        in_specs=[vmem] * 4,
        out_specs=(hbm, vmem, vmem),
        scratch_shapes=[
            pltpu.VMEM((n * depth, tile), jnp.float32),
            pltpu.VMEM((3, rows, tile), jnp.float32),
            dma((3,)),
        ],
        compiler_params=pltpu.CompilerParams(vmem_limit_bytes=16 << 20),
    )(old, rowt, rowd, colp)
    new_weight = pl.pallas_call(
        functools.partial(step_kernel, n, tile * n),
        out_shape=jax.ShapeDtypeStruct((depth, tile), jnp.float32),
        in_specs=[vmem] * 4,
        out_specs=vmem,
        scratch_shapes=[
            pltpu.VMEM((n, depth, tile), jnp.bfloat16),
            pltpu.VMEM((n, 8, 128), jnp.float32),
            dma((n - 1,)),
            dma((n * n - 1,)),
            dma((n,)),
            dma((n,)),
        ],
        compiler_params=pltpu.CompilerParams(
            collective_id=1, has_side_effects=True, vmem_limit_bytes=8 << 20
        ),
    )(partial.reshape(n, depth, tile), weight, block_mask, trace)
    return hessian, new_weight


def solution(mesh):
    n = mesh.shape["row"]

    def on_device(hessian_old, tokens, weight, dense_weight, block_mask):
        tile = hessian_old.shape[0]
        fits = (
            n == mesh.shape["col"]
            and n > 1
            and n % 2 == 0
            and tile == hessian_old.shape[1]
            and tile % 128 == 0
            and tile == block_mask.shape[1] * 128
            and tokens.shape[0] % 16 == 0
            and weight.shape[0] % 16 == 0
        )
        args = (hessian_old, tokens, weight, dense_weight, block_mask)
        return fused(n, *args) if fits else general(*args)

    spec = P(("grp", "row"), "col")
    return jax.shard_map(
        on_device, mesh=mesh, in_specs=(spec,) * 5, out_specs=(spec, spec), check_vma=False
    )
```
